32 devices in a mesh: gx: 2 (over x), gy: 16 (over z, y, core).
Axes of the slice: x: 2, y: 2, z: 4, core: 2. Of those that a mesh axis runs over, the one named last changes fastest.
Arguments:
- cell: int32 [1048576], P(('gx', 'gy')), may hold values from 0 to 524287
- vehicle: int32 [1048576], P(('gx', 'gy')), may hold values from 0 to 1023
- speed: float32 [1048576], P(('gx', 'gy')), may hold values from 0 to 64, as said below
Outputs:
- top_speed: float32 [524288], P(('gx', 'gy'))
- top_vehicle: int32 [524288], P(('gx', 'gy'))
The draws below stay inside these ranges and needn't reach their ends.
Inputs may be any that keep to these rules, and one draw needn't show every extreme that they name: Every speed is a whole multiple of 1/1024.
All inputs are finite; a program needn't handle non-finite values.
Results may differ from the reference program's by a relative error of at most 0.0003.
Values sent between devices are 32-bit elements; how exact they have to be, the bound alone decides.
A program may use at most 64 MiB of HBM per device.

```python
import math
import jax
import jax.numpy as jnp
import numpy as np

CELLS = 524288
VEHICLES = 1024
EVENTS = 1048576


def draw_speed(key, part):
    level_key = jax.random.fold_in(key, 11)
    plant_key = jax.random.fold_in(key, 23)
    levels = jax.random.randint(level_key, (EVENTS,), 0, 65537)
    values = levels.astype(jnp.float32) / 1024.0
    planted = jax.random.randint(plant_key, (EVENTS,), 0, 512)
    values = jnp.where(planted == 0, 64.0, values)
    return values.astype(jnp.float32)


def with_ends(entries, own_key, least, high):
    dims = entries.shape
    index_at = [jax.random.randint(jax.random.fold_in(own_key, axis), (), 0, dims[axis]) for axis in range(len(dims))]
    entries = entries.at[tuple(index_at)].set(least)
    longest = dims.index(max(dims))
    index_at[longest] = (index_at[longest] + 1) % dims[longest]
    return entries.at[tuple(index_at)].set(high)


def ranked_wide(own_key, extent, amount, slope):
    weights = [min(1 << octave, amount + 1 - (1 << octave)) * (1 << 20) // math.isqrt((1 << octave) ** slope) + 1 for octave in range((amount + 1).bit_length()) if 1 << octave <= amount]
    scale = 1 + sum(weights) // (1 << 30)
    listing = np.cumsum(np.array([max(1, weight // scale) for weight in weights]))
    ticket = jax.random.randint(jax.random.fold_in(own_key, 1), extent, 0, int(listing[len(weights) - 1]))
    start = jnp.left_shift(1, jnp.searchsorted(jnp.asarray(listing, jnp.int32), ticket, side="right").astype(jnp.int32))
    rank = start - 1 + jax.random.randint(jax.random.fold_in(own_key, 4), extent, 0, 1 << 30) % jnp.minimum(start, amount + 1 - start)
    return jax.random.permutation(jax.random.fold_in(own_key, 2), amount)[rank].astype(jnp.int32)


def setup_inputs(seed: int = 0) -> dict:
    splits = jax.random.split(jax.random.key(seed), 4)
    cell = with_ends(ranked_wide(splits[0], (EVENTS,), CELLS, 2), jax.random.fold_in(splits[0], 3), 0, CELLS - 1).astype(jnp.int32)
    vehicle = with_ends(jax.random.randint(splits[1], (EVENTS,), 0, VEHICLES), jax.random.fold_in(splits[1], 1), 0, VEHICLES - 1).astype(jnp.int32)
    speed = draw_speed(jax.random.fold_in(splits[3], 71), 0)
    return dict(cell=cell, vehicle=vehicle, speed=speed)


def reference(cell, vehicle, speed):
    top_speed = jnp.full((CELLS,), -1.0, jnp.float32).at[cell].max(speed)
    chosen = jnp.where(speed == top_speed[cell], vehicle, VEHICLES).astype(jnp.int32)
    lowest = jnp.full((CELLS,), VEHICLES, jnp.int32).at[cell].min(chosen)
    top_vehicle = jnp.where(lowest < VEHICLES, lowest, -1).astype(jnp.int32)
    return top_speed, top_vehicle
```

```python
import jax
import jax.numpy as jnp
from jax import lax
from jax.sharding import PartitionSpec as P

CELLS = 524288
TOP = 65536
UNIT = 1024
EMPTY = (TOP + UNIT) * UNIT


def swapped(block, axis, apart):
    count = lax.axis_size(axis)
    route = []
    for low in range(count):
        high = low | 1 << apart
        if high != low and high < count:
            route += [(low, high), (high, low)]
    return lax.ppermute(block, axis, route)


def encode(speed, vehicle):
    return (TOP - (speed * UNIT).astype(jnp.int32)) * UNIT + vehicle


def decode(code):
    level = TOP - (code >> 10)
    return level.astype(jnp.float32) * (1.0 / UNIT), code & (UNIT - 1)


def finish(code):
    speed, vehicle = decode(code)
    return speed, jnp.where(speed < 0, -1, vehicle)


def dense(cell, code):
    buffer = jnp.full((CELLS,), EMPTY, jnp.int32).at[cell].min(code)
    outer = lax.axis_size("gx")
    inner = lax.axis_size("gy")
    nbits = (outer * inner).bit_length() - 1
    myself = lax.axis_index(("gx", "gy"))
    for level in reversed(range(nbits)):
        half = buffer.shape[0] // 2
        side = myself >> level & 1
        keep = lax.dynamic_slice_in_dim(buffer, side * half, half, 0)
        give = lax.dynamic_slice_in_dim(buffer, (1 - side) * half, half, 0)
        speed, vehicle = decode(give)
        partner = swapped(jnp.stack([speed, vehicle.astype(jnp.float32)]), ("gx", "gy"), level)
        buffer = jnp.minimum(keep, encode(partner[0], partner[1].astype(jnp.int32)))
    return finish(buffer)


def per_device(cell, vehicle, speed):
    return dense(cell, encode(speed, vehicle))


def solution(mesh):
    placed = (P(("gx", "gy")), P(("gx", "gy")), P(("gx", "gy")))
    return jax.shard_map(
        per_device,
        mesh=mesh,
        in_specs=placed,
        out_specs=(P(("gx", "gy")), P(("gx", "gy"))),
        check_vma=False,
    )
```

```python
import functools

import jax
import jax.numpy as jnp
from jax import lax
from jax.experimental import pallas as pl
from jax.experimental.pallas import tpu as pltpu
from jax.sharding import PartitionSpec as P

CELLS = 524288
TOP = 65536
UNIT = 1024
EMPTY = (TOP + UNIT) * UNIT
NONE = 1 << 30
FAIL = -2
SUBS = 8
LANES = 128
WIDE = 4


def swapped(block, axis, apart):
    count = lax.axis_size(axis)
    route = []
    for low in range(count):
        high = low | 1 << apart
        if high != low and high < count:
            route += [(low, high), (high, low)]
    return lax.ppermute(block, axis, route)


def encode(speed, vehicle):
    return (TOP - (speed * UNIT).astype(jnp.int32)) * UNIT + vehicle


def decode(code):
    level = TOP - (code >> 10)
    return level.astype(jnp.float32) * (1.0 / UNIT), code & (UNIT - 1)


def finish(code):
    speed, vehicle = decode(code)
    return speed, jnp.where(speed < 0, -1, vehicle)


def dense(cell, vehicle, speed):
    code = encode(speed, vehicle)
    buffer = jnp.full((CELLS,), EMPTY, jnp.int32).at[cell].min(code)
    outer = lax.axis_size("gx")
    inner = lax.axis_size("gy")
    nbits = (outer * inner).bit_length() - 1
    myself = lax.axis_index(("gx", "gy"))
    for level in reversed(range(nbits)):
        half = buffer.shape[0] // 2
        side = myself >> level & 1
        keep = lax.dynamic_slice_in_dim(buffer, side * half, half, 0)
        give = lax.dynamic_slice_in_dim(buffer, (1 - side) * half, half, 0)
        speed, vehicle = decode(give)
        partner = swapped(jnp.stack([speed, vehicle.astype(jnp.float32)]), ("gx", "gy"), level)
        buffer = jnp.minimum(keep, encode(partner[0], partner[1].astype(jnp.int32)))
    return finish(buffer)


def lane_of():
    return lax.broadcasted_iota(jnp.int32, (SUBS, LANES), 1)


def sub_of():
    return lax.broadcasted_iota(jnp.int32, (SUBS, LANES), 0)


def before(c, k, pc, pk):
    return (c < pc) | ((c == pc) & (k < pk))


def exchange(c, k, pc, pk, high):
    keep = jnp.logical_xor(before(c, k, pc, pk), high)
    return jnp.where(keep, c, pc), jnp.where(keep, k, pk)


def pair(x, y):
    swap = before(y[0], y[1], x[0], x[1])
    low = jnp.where(swap, y[0], x[0]), jnp.where(swap, y[1], x[1])
    high = jnp.where(swap, x[0], y[0]), jnp.where(swap, x[1], y[1])
    return low, high


def turned(bit, vbits):
    place = lane_of() * SUBS + sub_of()
    return -((place >> (bit - vbits)) & 1)


def merge_vregs(cs, ks, flip):
    v = cs.shape[0]
    half = v // 2
    for i in range(half):
        a, b = pair((cs[i], ks[i]), (cs[i + half], ks[i + half]))
        cs[i], ks[i] = a
        cs[i + half], ks[i + half] = b
    for base in (0, half):
        x = [(cs[base + i], ks[base + i]) for i in range(half)]
        stride = half // 2
        while stride:
            for i in range(half):
                if not i & stride:
                    x[i], x[i + stride] = pair(x[i], x[i + stride])
            stride //= 2
        for i in range(half):
            cs[base + i] = x[i][0] ^ flip
            ks[base + i] = x[i][1] ^ flip


def sort(cs, ks):
    v = cs.shape[0]
    half = v // 2
    vbits = v.bit_length() - 1
    total = vbits + 10
    flip = turned(vbits, vbits)
    for base in (0, half):
        x = [(cs[base + i] ^ flip, ks[base + i] ^ flip) for i in range(half)]
        for phase in range(1, vbits):
            stride = 1 << (phase - 1)
            while stride:
                for i in range(half):
                    if not i & stride:
                        a, b = pair(x[i], x[i + stride])
                        if (base + i) >> phase & 1:
                            a, b = b, a
                        x[i], x[i + stride] = a, b
                stride //= 2
        for i in range(half):
            cs[base + i], ks[base + i] = x[i]
    merge_vregs(cs, ks, turned(vbits, vbits) ^ turned(vbits + 1, vbits))
    lane = lane_of()
    sub = sub_of()

    def sub_stage(j):
        step = 1 << j
        high = (sub & step) != 0

        def partner(x):
            up = pltpu.roll(x, step, 0)
            if step * 2 == SUBS:
                return up
            return jnp.where(high, up, pltpu.roll(x, SUBS - step, 0))

        for i in range(v):
            c, k = cs[i], ks[i]
            cs[i], ks[i] = exchange(c, k, partner(c), partner(k), high)

    def lane_stage(n, bits):
        step = jnp.int32(1) << (bits - 1 - n)
        high = (lane & step) != 0
        source = lane ^ step

        def partner(x):
            return jnp.take_along_axis(x, source, axis=1, mode="promise_in_bounds")

        for i in range(v):
            c, k = cs[i], ks[i]
            cs[i], ks[i] = exchange(c, k, partner(c), partner(k), high)
        return bits

    def phase_body(phase, carry):
        bits = jnp.maximum(phase - vbits - 3, 0)
        lax.fori_loop(0, bits, lane_stage, bits)
        for j in (2, 1, 0):
            pl.when(phase - vbits - 1 >= j)(functools.partial(sub_stage, j))
        merge_vregs(cs, ks, turned(phase, vbits) ^ turned(phase + 1, vbits))
        return carry

    lax.fori_loop(vbits + 1, total + 1, phase_body, 0)


def earlier(x, q):
    y = pltpu.roll(x, q, 0)
    return jnp.where(sub_of() < q, pltpu.roll(y, 1, 1), y)


def later(x, q):
    y = pltpu.roll(x, SUBS - q, 0)
    return jnp.where(sub_of() >= SUBS - q, pltpu.roll(y, LANES - 1, 1), y)


def compress(cs, ks, ds, cs2, ks2, ds2):
    v = cs.shape[0]
    vbits = v.bit_length() - 1
    lane = lane_of()
    sub = sub_of()
    start = (lane == 0) & (sub == 0)
    count = jnp.zeros((SUBS, LANES), jnp.int32)
    last = jnp.where(start, -1, earlier(cs[v - 1], 1))
    for i in range(v):
        c = cs[i]
        lost = (c == last) | (c >= NONE)
        ds[i] = jnp.where(lost, -1, count)
        count = count + lost.astype(jnp.int32)
        last = c
    scan = count
    for q in (1, 2, 4):
        scan = scan + jnp.where(sub >= q, pltpu.roll(scan, q, 0), 0)
    column = jnp.broadcast_to(scan[SUBS - 1 : SUBS, :], (SUBS, LANES))
    run = column
    for q in (1, 2, 4, 8, 16, 32, 64):
        run = run + jnp.where(lane >= q, pltpu.roll(run, q, 1), 0)
    offset = run - column + scan - count
    for i in range(v):
        d = ds[i]
        cs[i] = jnp.where(d < 0, NONE, cs[i])
        ds[i] = jnp.where(d < 0, 0, d + offset)

    def step(own, inc, bit):
        c, k, d = own
        pc, pk, pd = inc
        comes = (pd & bit) != 0
        goes = (d & bit) != 0
        return (
            jnp.where(comes, pc, jnp.where(goes, NONE, c)),
            jnp.where(comes, pk, k),
            jnp.where(comes, pd, jnp.where(goes, 0, d)),
        )

    now, then = (cs, ks, ds), (cs2, ks2, ds2)
    for b in range(vbits):
        for i in range(v):
            j = i + (1 << b)
            own = tuple(r[i] for r in now)
            inc = tuple(r[j] if j < v else later(r[j - v], 1) for r in now)
            for r, x in zip(then, step(own, inc, 1 << b)):
                r[i] = x
        now, then = then, now
    for b in range(3):
        for i in range(v):
            own = tuple(r[i] for r in now)
            inc = tuple(later(x, 1 << b) for x in own)
            for r, x in zip(now, step(own, inc, 1 << (b + vbits))):
                r[i] = x

    def lane_step(b, carry):
        shift = LANES - (jnp.int32(1) << b)
        for i in range(v):
            own = tuple(r[i] for r in now)
            inc = tuple(pltpu.roll(x, shift, 1) for x in own)
            for r, x in zip(now, step(own, inc, jnp.int32(1) << (b + vbits + 3))):
                r[i] = x
        return carry

    lax.fori_loop(0, 7, lane_step, 0)
    return now, then


def expand(ks, ds, ks2, ds2):
    v = ks.shape[0]
    vbits = v.bit_length() - 1

    def step(own, inc, bit):
        k, d = own
        pk, pd = inc
        comes = (pd & bit) != 0
        goes = (d & bit) != 0
        return (
            jnp.where(comes, pk, jnp.where(goes, EMPTY, k)),
            jnp.where(comes, pd, jnp.where(goes, 0, d)),
        )

    now, then = (ks, ds), (ks2, ds2)

    def lane_step(n, carry):
        b = 6 - n
        for i in range(v):
            own = tuple(r[i] for r in now)
            inc = tuple(pltpu.roll(x, jnp.int32(1) << b, 1) for x in own)
            for r, x in zip(now, step(own, inc, jnp.int32(1) << (b + vbits + 3))):
                r[i] = x
        return carry

    lax.fori_loop(0, 7, lane_step, 0)
    for b in (2, 1, 0):
        for i in range(v):
            own = tuple(r[i] for r in now)
            inc = tuple(earlier(x, 1 << b) for x in own)
            for r, x in zip(now, step(own, inc, 1 << (b + vbits))):
                r[i] = x
    for b in reversed(range(vbits)):
        for i in range(v):
            j = i - (1 << b)
            own = tuple(r[i] for r in now)
            inc = tuple(r[j] if j >= 0 else earlier(r[j + v], 1) for r in now)
            for r, x in zip(then, step(own, inc, 1 << b)):
                r[i] = x
        now, then = then, now
    return now[0]


def send_kernel(n, cell_ref, vehicle_ref, speed_ref, out_ref, cs, ks, ds, cs2, ks2, ds2, tc, tk):
    v = cs.shape[0]
    own = CELLS // n
    for i in range(v):
        cs[i] = cell_ref[i]
        ks[i] = encode(speed_ref[i], vehicle_ref[i])
    sort(cs, ks)
    (c, k, _), _ = compress(cs, ks, ds, cs2, ks2, ds2)
    first = c[0][0:1, :]
    parts = SUBS // WIDE
    rows = v // parts
    for h in range(parts):
        tc[h] = jnp.transpose(c[h * rows : (h + 1) * rows].reshape(rows * SUBS, LANES))
        tk[h] = jnp.transpose(k[h * rows : (h + 1) * rows].reshape(rows * SUBS, LANES))
    ahead = [jnp.sum((first < o * own).astype(jnp.int32)) for o in range(n + 1)]
    starts = [jnp.clip(ahead[o] - 1, 0, LANES - WIDE) for o in range(n)]
    fails = jnp.int32(0)
    for o in range(n):
        fails = fails | (ahead[o + 1] > starts[o] + WIDE).astype(jnp.int32)
    for o in range(n):
        for h in range(parts):
            c = tc[h, pl.ds(starts[o], WIDE), :]
            k = tk[h, pl.ds(starts[o], WIDE), :]
            at = h * WIDE
            out_ref[o, at : at + WIDE, :] = jnp.where(fails > 0, FAIL, c)
            out_ref[o, SUBS + at : SUBS + at + WIDE, :] = TOP - (k >> 10)
            out_ref[o, 2 * SUBS + at : 2 * SUBS + at + WIDE, :] = k & (UNIT - 1)


def owner_kernel(n, got_ref, speed_ref, vehicle_ref, fail_ref, cs, ks, ds, cs2, ks2, ds2, tall):
    v = cs.shape[0]
    vbits = v.bit_length() - 1
    own = CELLS // n
    base = (lax.axis_index("gx") * lax.axis_size("gy") + lax.axis_index("gy")) * own
    least = jnp.zeros((SUBS, LANES), jnp.int32)
    for i in range(v):
        c = got_ref[i, 0:SUBS, :]
        least = jnp.minimum(least, c)
        c = c - base
        cs[i] = jnp.where((c >= 0) & (c < own), c, NONE)
        ks[i] = (TOP - got_ref[i, SUBS : 2 * SUBS, :]) * UNIT + got_ref[i, 2 * SUBS : 3 * SUBS, :]
    fail_ref[...] = least
    sort(cs, ks)
    (c, k, d), (_, k2, d2) = compress(cs, ks, ds, cs2, ks2, ds2)
    place = (lane_of() * SUBS + sub_of()) * v
    for i in range(v):
        empty = c[i] >= NONE
        d[i] = jnp.where(empty, 0, c[i] - (place + i))
        k[i] = jnp.where(empty, EMPTY, k[i])
    done = expand(k, d, k2, d2)
    for i in range(v):
        tall[pl.Slice(i, SUBS, v), :] = done[i]
    columns = own // (v * SUBS)
    parts = v * SUBS // LANES
    wide = jnp.transpose(tall[...])
    for h in range(parts):
        speed, vehicle = finish(wide[0:columns, h * LANES : (h + 1) * LANES])
        speed_ref[pl.Slice(h, columns, parts), :] = speed
        vehicle_ref[pl.Slice(h, columns, parts), :] = vehicle


def sparse(cell, vehicle, speed, n):
    v = cell.shape[0] // (SUBS * LANES)
    own = CELLS // n
    shape = (v, SUBS, LANES)
    slots = [pltpu.VMEM(shape, jnp.int32)] * 6
    turn = pltpu.VMEM((SUBS // WIDE, LANES, v * WIDE), jnp.int32)
    sent = pl.pallas_call(
        functools.partial(send_kernel, n),
        out_shape=jax.ShapeDtypeStruct((n, 3 * SUBS, LANES), jnp.int32),
        scratch_shapes=slots + [turn, turn],
    )(cell.reshape(shape), vehicle.reshape(shape), speed.reshape(shape))
    got = lax.all_to_all(sent, ("gx", "gy"), 0, 0)
    best, ident, least = pl.pallas_call(
        functools.partial(owner_kernel, n),
        out_shape=(
            jax.ShapeDtypeStruct((own // LANES, LANES), jnp.float32),
            jax.ShapeDtypeStruct((own // LANES, LANES), jnp.int32),
            jax.ShapeDtypeStruct((SUBS, LANES), jnp.int32),
        ),
        scratch_shapes=slots + [pltpu.VMEM((v * SUBS, LANES), jnp.int32)],
    )(got)
    return best.reshape(own), ident.reshape(own), jnp.min(least) < 0


def per_device(cell, vehicle, speed):
    n = lax.axis_size("gx") * lax.axis_size("gy")
    v = cell.shape[0] // (SUBS * LANES)
    if v != n or v * WIDE != LANES or cell.shape[0] % (SUBS * LANES) or CELLS % (n * v * SUBS):
        return dense(cell, vehicle, speed)
    best, ident, failed = sparse(cell, vehicle, speed, n)
    return lax.cond(
        failed,
        lambda: dense(cell, vehicle, speed),
        lambda: (best, ident),
    )


def solution(mesh):
    placed = (P(("gx", "gy")), P(("gx", "gy")), P(("gx", "gy")))
    return jax.shard_map(
        per_device,
        mesh=mesh,
        in_specs=placed,
        out_specs=(P(("gx", "gy")), P(("gx", "gy"))),
        check_vma=False,
    )
```

```python
import functools

import jax
import jax.numpy as jnp
from jax import lax
from jax.experimental import pallas as pl
from jax.experimental.pallas import tpu as pltpu
from jax.sharding import PartitionSpec as P

CELLS = 524288
TOP = 65536
UNIT = 1024
EMPTY = (TOP + UNIT) * UNIT
NONE = 1 << 30
FAIL = -2000000000
SUBS = 8
LANES = 128
WIDE = 4


def swapped(block, axis, apart):
    count = lax.axis_size(axis)
    route = []
    for low in range(count):
        high = low | 1 << apart
        if high != low and high < count:
            route += [(low, high), (high, low)]
    return lax.ppermute(block, axis, route)


def encode(speed, vehicle):
    return (TOP - (speed * UNIT).astype(jnp.int32)) * UNIT + vehicle


def decode(code):
    level = TOP - (code >> 10)
    return level.astype(jnp.float32) * (1.0 / UNIT), code & (UNIT - 1)


def finish(code):
    speed, vehicle = decode(code)
    return speed, jnp.where(speed < 0, -1, vehicle)


def dense(cell, vehicle, speed):
    code = encode(speed, vehicle)
    buffer = jnp.full((CELLS,), EMPTY, jnp.int32).at[cell].min(code)
    outer = lax.axis_size("gx")
    inner = lax.axis_size("gy")
    nbits = (outer * inner).bit_length() - 1
    myself = lax.axis_index(("gx", "gy"))
    for level in reversed(range(nbits)):
        half = buffer.shape[0] // 2
        side = myself >> level & 1
        keep = lax.dynamic_slice_in_dim(buffer, side * half, half, 0)
        give = lax.dynamic_slice_in_dim(buffer, (1 - side) * half, half, 0)
        speed, vehicle = decode(give)
        partner = swapped(jnp.stack([speed, vehicle.astype(jnp.float32)]), ("gx", "gy"), level)
        buffer = jnp.minimum(keep, encode(partner[0], partner[1].astype(jnp.int32)))
    return finish(buffer)


def lane_of():
    return lax.broadcasted_iota(jnp.int32, (SUBS, LANES), 1)


def sub_of():
    return lax.broadcasted_iota(jnp.int32, (SUBS, LANES), 0)


def before(c, k, pc, pk):
    return (c < pc) | ((c == pc) & (k < pk))


def exchange(c, k, pc, pk, high):
    keep = jnp.logical_xor(before(c, k, pc, pk), high)
    return jnp.where(keep, c, pc), jnp.where(keep, k, pk)


def pair(x, y):
    swap = before(y[0], y[1], x[0], x[1])
    low = jnp.where(swap, y[0], x[0]), jnp.where(swap, y[1], x[1])
    high = jnp.where(swap, x[0], y[0]), jnp.where(swap, x[1], y[1])
    return low, high


def turned(bit, vbits):
    place = lane_of() * SUBS + sub_of()
    return -((place >> (bit - vbits)) & 1)


def merge_vregs(cs, ks, flip):
    v = cs.shape[0]
    half = v // 2
    for i in range(half):
        a, b = pair((cs[i], ks[i]), (cs[i + half], ks[i + half]))
        cs[i], ks[i] = a
        cs[i + half], ks[i + half] = b
    for base in (0, half):
        x = [(cs[base + i], ks[base + i]) for i in range(half)]
        stride = half // 2
        while stride:
            for i in range(half):
                if not i & stride:
                    x[i], x[i + stride] = pair(x[i], x[i + stride])
            stride //= 2
        for i in range(half):
            cs[base + i] = x[i][0] ^ flip
            ks[base + i] = x[i][1] ^ flip


def sort(cs, ks):
    v = cs.shape[0]
    half = v // 2
    vbits = v.bit_length() - 1
    total = vbits + 10
    flip = turned(vbits, vbits)
    for base in (0, half):
        x = [(cs[base + i] ^ flip, ks[base + i] ^ flip) for i in range(half)]
        for phase in range(1, vbits):
            stride = 1 << (phase - 1)
            while stride:
                for i in range(half):
                    if not i & stride:
                        a, b = pair(x[i], x[i + stride])
                        if (base + i) >> phase & 1:
                            a, b = b, a
                        x[i], x[i + stride] = a, b
                stride //= 2
        for i in range(half):
            cs[base + i], ks[base + i] = x[i]
    merge_vregs(cs, ks, turned(vbits, vbits) ^ turned(vbits + 1, vbits))
    merge_phases(cs, ks, vbits + 1)


def merge_phases(cs, ks, begin):
    v = cs.shape[0]
    vbits = v.bit_length() - 1
    total = vbits + 10
    lane = lane_of()
    sub = sub_of()

    def sub_stage(j):
        step = 1 << j
        high = (sub & step) != 0

        def partner(x):
            up = pltpu.roll(x, step, 0)
            if step * 2 == SUBS:
                return up
            return jnp.where(high, up, pltpu.roll(x, SUBS - step, 0))

        for i in range(v):
            c, k = cs[i], ks[i]
            cs[i], ks[i] = exchange(c, k, partner(c), partner(k), high)

    def lane_stage(n, bits):
        step = jnp.int32(1) << (bits - 1 - n)
        high = (lane & step) != 0
        source = lane ^ step

        def partner(x):
            return jnp.take_along_axis(x, source, axis=1, mode="promise_in_bounds")

        for i in range(v):
            c, k = cs[i], ks[i]
            cs[i], ks[i] = exchange(c, k, partner(c), partner(k), high)
        return bits

    def phase_body(phase, carry):
        bits = jnp.maximum(phase - vbits - 3, 0)
        lax.fori_loop(0, bits, lane_stage, bits)
        for j in (2, 1, 0):
            if begin - vbits - 1 >= j:
                sub_stage(j)
            else:
                pl.when(phase - vbits - 1 >= j)(functools.partial(sub_stage, j))
        merge_vregs(cs, ks, turned(phase, vbits) ^ turned(phase + 1, vbits))
        return carry

    lax.fori_loop(begin, total + 1, phase_body, 0)


def earlier(x, q):
    y = pltpu.roll(x, q, 0)
    return jnp.where(sub_of() < q, pltpu.roll(y, 1, 1), y)


def later(x, q):
    y = pltpu.roll(x, SUBS - q, 0)
    return jnp.where(sub_of() >= SUBS - q, pltpu.roll(y, LANES - 1, 1), y)


def compress(limit, cs, ks, ds, cs2, ks2, ds2):
    v = cs.shape[0]
    vbits = v.bit_length() - 1
    lane = lane_of()
    sub = sub_of()
    start = (lane == 0) & (sub == 0)
    count = jnp.zeros((SUBS, LANES), jnp.int32)
    last = jnp.where(start, FAIL, earlier(cs[v - 1], 1))
    for i in range(v):
        c = cs[i]
        lost = (c == last) | (c < 0) | (c >= limit)
        ds[i] = jnp.where(lost, -1, count)
        count = count + lost.astype(jnp.int32)
        last = c
    scan = count
    for q in (1, 2, 4):
        scan = scan + jnp.where(sub >= q, pltpu.roll(scan, q, 0), 0)
    column = jnp.broadcast_to(scan[SUBS - 1 : SUBS, :], (SUBS, LANES))
    run = column
    for q in (1, 2, 4, 8, 16, 32, 64):
        run = run + jnp.where(lane >= q, pltpu.roll(run, q, 1), 0)
    offset = run - column + scan - count
    for i in range(v):
        d = ds[i]
        cs[i] = jnp.where(d < 0, NONE, cs[i])
        ds[i] = jnp.where(d < 0, 0, d + offset)

    def step(own, inc, bit):
        c, k, d = own
        pc, pk, pd = inc
        comes = (pd & bit) != 0
        goes = (d & bit) != 0
        return (
            jnp.where(comes, pc, jnp.where(goes, NONE, c)),
            jnp.where(comes, pk, k),
            jnp.where(comes, pd, jnp.where(goes, 0, d)),
        )

    now, then = (cs, ks, ds), (cs2, ks2, ds2)
    for b in range(vbits):
        for i in range(v):
            j = i + (1 << b)
            own = tuple(r[i] for r in now)
            inc = tuple(r[j] if j < v else later(r[j - v], 1) for r in now)
            for r, x in zip(then, step(own, inc, 1 << b)):
                r[i] = x
        now, then = then, now
    for b in range(3):
        for i in range(v):
            own = tuple(r[i] for r in now)
            inc = tuple(later(x, 1 << b) for x in own)
            for r, x in zip(now, step(own, inc, 1 << (b + vbits))):
                r[i] = x

    def lane_step(b, carry):
        shift = LANES - (jnp.int32(1) << b)
        for i in range(v):
            own = tuple(r[i] for r in now)
            inc = tuple(pltpu.roll(x, shift, 1) for x in own)
            for r, x in zip(now, step(own, inc, jnp.int32(1) << (b + vbits + 3))):
                r[i] = x
        return carry

    lax.fori_loop(0, 7, lane_step, 0)
    return now, then


def expand(ks, ds, ks2, ds2):
    v = ks.shape[0]
    vbits = v.bit_length() - 1

    def step(own, inc, bit):
        k, d = own
        pk, pd = inc
        comes = (pd & bit) != 0
        goes = (d & bit) != 0
        return (
            jnp.where(comes, pk, jnp.where(goes, EMPTY, k)),
            jnp.where(comes, pd, jnp.where(goes, 0, d)),
        )

    now, then = (ks, ds), (ks2, ds2)

    def lane_step(n, carry):
        b = 6 - n
        for i in range(v):
            own = tuple(r[i] for r in now)
            inc = tuple(pltpu.roll(x, jnp.int32(1) << b, 1) for x in own)
            for r, x in zip(now, step(own, inc, jnp.int32(1) << (b + vbits + 3))):
                r[i] = x
        return carry

    lax.fori_loop(0, 7, lane_step, 0)
    for b in (2, 1, 0):
        for i in range(v):
            own = tuple(r[i] for r in now)
            inc = tuple(earlier(x, 1 << b) for x in own)
            for r, x in zip(now, step(own, inc, 1 << (b + vbits))):
                r[i] = x
    for b in reversed(range(vbits)):
        for i in range(v):
            j = i - (1 << b)
            own = tuple(r[i] for r in now)
            inc = tuple(r[j] if j >= 0 else earlier(r[j + v], 1) for r in now)
            for r, x in zip(then, step(own, inc, 1 << b)):
                r[i] = x
        now, then = then, now
    return now[0]


def myself():
    return lax.axis_index("gx") * lax.axis_size("gy") + lax.axis_index("gy")


def send_kernel(n, cell_ref, vehicle_ref, speed_ref, out_ref, cs, ks, ds, cs2, ks2, ds2, tc, tk):
    v = cs.shape[0]
    own = CELLS // n
    odd = myself() & 1
    for i in range(v):
        c = cell_ref[i]
        cs[i] = jnp.where(odd == 1, CELLS - 1 - c, c)
        ks[i] = encode(speed_ref[i], vehicle_ref[i])
    sort(cs, ks)
    (c, k, _), _ = compress(CELLS, cs, ks, ds, cs2, ks2, ds2)
    first = c[0][0:1, :]
    parts = SUBS // WIDE
    rows = v // parts
    for h in range(parts):
        tc[h] = jnp.transpose(c[h * rows : (h + 1) * rows].reshape(rows * SUBS, LANES))
        tk[h] = jnp.transpose(k[h * rows : (h + 1) * rows].reshape(rows * SUBS, LANES))
    ahead = [jnp.sum((first < o * own).astype(jnp.int32)) for o in range(n + 1)]
    starts = [jnp.clip(ahead[o] - 1, 0, LANES - WIDE) for o in range(n)]
    fails = jnp.int32(0)
    for o in range(n):
        fails = fails | (ahead[o + 1] > starts[o] + WIDE).astype(jnp.int32)
    for q in range(n):
        o = jnp.where(odd == 1, n - 1 - q, q)
        for h in range(parts):
            c = tc[h, pl.ds(starts[q], WIDE), :]
            k = jnp.where(c >= NONE, 0, tk[h, pl.ds(starts[q], WIDE), :])
            c = jnp.where(odd == 1, CELLS - 1 - c, c)
            at = h * WIDE
            out_ref[o, at : at + WIDE, :] = jnp.where(fails > 0, FAIL, c)
            out_ref[o, SUBS + at : SUBS + at + WIDE, :] = TOP - (k >> 10)
            out_ref[o, 2 * SUBS + at : 2 * SUBS + at + WIDE, :] = k & (UNIT - 1)


def swap_kernel(n, sent, got, send_sem, recv_sem):
    me = myself()
    inner = lax.axis_size("gy")

    def spot(device):
        return (device // inner, device % inner)

    barrier = pltpu.get_barrier_semaphore()
    for k in range(1, n):
        pl.semaphore_signal(barrier, inc=1, device_id=spot(me ^ k), device_id_type=pl.DeviceIdType.MESH)
    mine = pltpu.make_async_copy(sent.at[me], got.at[me], send_sem.at[0])
    mine.start()
    pl.semaphore_wait(barrier, n - 1)
    copies = []
    for k in range(1, n):
        copy = pltpu.make_async_remote_copy(
            src_ref=sent.at[me ^ k],
            dst_ref=got.at[me],
            send_sem=send_sem.at[k],
            recv_sem=recv_sem.at[k],
            device_id=spot(me ^ k),
            device_id_type=pl.DeviceIdType.MESH,
        )
        copy.start()
        copies.append(copy)
    mine.wait()
    for copy in copies:
        copy.wait()


def owner_kernel(n, got_ref, speed_ref, vehicle_ref, fail_ref, cs, ks, ds, cs2, ks2, ds2, tall):
    v = cs.shape[0]
    vbits = v.bit_length() - 1
    own = CELLS // n
    base = myself() * own
    parts = SUBS // WIDE
    rows = v // parts
    begin = vbits + 3 + WIDE.bit_length()
    flip = turned(begin, vbits)
    least = jnp.zeros((SUBS, LANES), jnp.int32)
    for h in range(parts):
        at = h * WIDE
        c = got_ref[:, at : at + WIDE, :].reshape(v * WIDE, LANES)
        level = got_ref[:, SUBS + at : SUBS + at + WIDE, :].reshape(v * WIDE, LANES)
        vehicle = got_ref[:, 2 * SUBS + at : 2 * SUBS + at + WIDE, :].reshape(v * WIDE, LANES)
        k = (TOP - level) * UNIT + vehicle
        least = jnp.minimum(least, jnp.min(c.reshape(v * WIDE // SUBS, SUBS, LANES), axis=0))
        c = jnp.transpose(c - base).reshape(rows, SUBS, LANES)
        k = jnp.transpose(k).reshape(rows, SUBS, LANES)
        for i in range(rows):
            cs[h * rows + i] = c[i] ^ flip
            ks[h * rows + i] = k[i] ^ flip
    fail_ref[0] = (jnp.min(least) == FAIL).astype(jnp.int32)
    merge_phases(cs, ks, begin)
    (c, k, d), (_, k2, d2) = compress(own, cs, ks, ds, cs2, ks2, ds2)
    place = (lane_of() * SUBS + sub_of()) * v
    for i in range(v):
        empty = c[i] >= NONE
        d[i] = jnp.where(empty, 0, c[i] - (place + i))
        k[i] = jnp.where(empty, EMPTY, k[i])
    done = expand(k, d, k2, d2)
    for i in range(v):
        tall[pl.Slice(i, SUBS, v), :] = done[i]
    columns = own // (v * SUBS)
    parts = v * SUBS // LANES
    wide = jnp.transpose(tall[...])
    for h in range(parts):
        speed, vehicle = finish(wide[0:columns, h * LANES : (h + 1) * LANES])
        speed_ref[pl.Slice(h, columns, parts), :] = speed
        vehicle_ref[pl.Slice(h, columns, parts), :] = vehicle


def sparse(cell, vehicle, speed, n):
    v = cell.shape[0] // (SUBS * LANES)
    own = CELLS // n
    shape = (v, SUBS, LANES)
    slots = [pltpu.VMEM(shape, jnp.int32)] * 6
    turn = pltpu.VMEM((SUBS // WIDE, LANES, v * WIDE), jnp.int32)
    sent = pl.pallas_call(
        functools.partial(send_kernel, n),
        out_shape=jax.ShapeDtypeStruct((n, 3 * SUBS, LANES), jnp.int32),
        scratch_shapes=slots + [turn, turn],
    )(cell.reshape(shape), vehicle.reshape(shape), speed.reshape(shape))
    got = pl.pallas_call(
        functools.partial(swap_kernel, n),
        out_shape=jax.ShapeDtypeStruct(sent.shape, sent.dtype),
        in_specs=[pl.BlockSpec(memory_space=pltpu.VMEM)],
        out_specs=pl.BlockSpec(memory_space=pltpu.VMEM),
        scratch_shapes=[
            pltpu.SemaphoreType.DMA((n,)),
            pltpu.SemaphoreType.DMA((n,)),
        ],
        compiler_params=pltpu.CompilerParams(collective_id=0, has_side_effects=True),
    )(sent)
    best, ident, fail = pl.pallas_call(
        functools.partial(owner_kernel, n),
        out_shape=(
            jax.ShapeDtypeStruct((own // LANES, LANES), jnp.float32),
            jax.ShapeDtypeStruct((own // LANES, LANES), jnp.int32),
            jax.ShapeDtypeStruct((1,), jnp.int32),
        ),
        out_specs=(
            pl.BlockSpec(memory_space=pltpu.VMEM),
            pl.BlockSpec(memory_space=pltpu.VMEM),
            pl.BlockSpec(memory_space=pltpu.SMEM),
        ),
        scratch_shapes=slots + [pltpu.VMEM((v * SUBS, LANES), jnp.int32)],
    )(got)
    return best.reshape(own), ident.reshape(own), fail[0] > 0


def per_device(cell, vehicle, speed):
    n = lax.axis_size("gx") * lax.axis_size("gy")
    v = cell.shape[0] // (SUBS * LANES)
    if v != n or v * WIDE != LANES or cell.shape[0] % (SUBS * LANES) or CELLS % (n * v * SUBS):
        return dense(cell, vehicle, speed)
    best, ident, failed = sparse(cell, vehicle, speed, n)
    return lax.cond(
        failed,
        lambda: dense(cell, vehicle, speed),
        lambda: (best, ident),
    )


def solution(mesh):
    placed = (P(("gx", "gy")), P(("gx", "gy")), P(("gx", "gy")))
    return jax.shard_map(
        per_device,
        mesh=mesh,
        in_specs=placed,
        out_specs=(P(("gx", "gy")), P(("gx", "gy"))),
        check_vma=False,
    )
```

```python
import functools

import jax
import jax.numpy as jnp
from jax import lax
from jax.experimental import pallas as pl
from jax.experimental.pallas import tpu as pltpu
from jax.sharding import PartitionSpec as P

CELLS = 524288
TOP = 65536
UNIT = 1024
EMPTY = (TOP + UNIT) * UNIT
NONE = 1 << 30
FAIL = -2000000000
SUBS = 8
LANES = 128
WIDE = 4
ROWS = 5
ORDER = (0, 2, 4, 1, 3)


def swapped(block, axis, apart):
    count = lax.axis_size(axis)
    route = []
    for low in range(count):
        high = low | 1 << apart
        if high != low and high < count:
            route += [(low, high), (high, low)]
    return lax.ppermute(block, axis, route)


def encode(speed, vehicle):
    return (TOP - (speed * UNIT).astype(jnp.int32)) * UNIT + vehicle


def decode(code):
    level = TOP - (code >> 10)
    return level.astype(jnp.float32) * (1.0 / UNIT), code & (UNIT - 1)


def finish(code):
    speed, vehicle = decode(code)
    return speed, jnp.where(speed < 0, -1, vehicle)


def dense(cell, vehicle, speed):
    code = encode(speed, vehicle)
    buffer = jnp.full((CELLS,), EMPTY, jnp.int32).at[cell].min(code)
    outer = lax.axis_size("gx")
    inner = lax.axis_size("gy")
    nbits = (outer * inner).bit_length() - 1
    myself = lax.axis_index(("gx", "gy"))
    for level in reversed(range(nbits)):
        half = buffer.shape[0] // 2
        side = myself >> level & 1
        keep = lax.dynamic_slice_in_dim(buffer, side * half, half, 0)
        give = lax.dynamic_slice_in_dim(buffer, (1 - side) * half, half, 0)
        speed, vehicle = decode(give)
        partner = swapped(jnp.stack([speed, vehicle.astype(jnp.float32)]), ("gx", "gy"), level)
        buffer = jnp.minimum(keep, encode(partner[0], partner[1].astype(jnp.int32)))
    return finish(buffer)


def lane_of():
    return lax.broadcasted_iota(jnp.int32, (SUBS, LANES), 1)


def sub_of():
    return lax.broadcasted_iota(jnp.int32, (SUBS, LANES), 0)


def before(c, k, pc, pk):
    return (c < pc) | ((c == pc) & (k < pk))


def exchange(c, k, pc, pk, high):
    keep = jnp.logical_xor(before(c, k, pc, pk), high)
    return jnp.where(keep, c, pc), jnp.where(keep, k, pk)


def pair(x, y):
    swap = before(y[0], y[1], x[0], x[1])
    low = jnp.where(swap, y[0], x[0]), jnp.where(swap, y[1], x[1])
    high = jnp.where(swap, x[0], y[0]), jnp.where(swap, x[1], y[1])
    return low, high


def turned(bit, vbits):
    place = lane_of() * SUBS + sub_of()
    return -((place >> (bit - vbits)) & 1)


def merge_vregs(cs, ks, flip):
    v = cs.shape[0]
    half = v // 2
    for i in range(half):
        a, b = pair((cs[i], ks[i]), (cs[i + half], ks[i + half]))
        cs[i], ks[i] = a
        cs[i + half], ks[i + half] = b
    for base in (0, half):
        x = [(cs[base + i], ks[base + i]) for i in range(half)]
        stride = half // 2
        while stride:
            for i in range(half):
                if not i & stride:
                    x[i], x[i + stride] = pair(x[i], x[i + stride])
            stride //= 2
        for i in range(half):
            cs[base + i] = x[i][0] ^ flip
            ks[base + i] = x[i][1] ^ flip


def sort(cs, ks):
    v = cs.shape[0]
    half = v // 2
    vbits = v.bit_length() - 1
    total = vbits + 10
    flip = turned(vbits, vbits)
    for base in (0, half):
        x = [(cs[base + i] ^ flip, ks[base + i] ^ flip) for i in range(half)]
        for phase in range(1, vbits):
            stride = 1 << (phase - 1)
            while stride:
                for i in range(half):
                    if not i & stride:
                        a, b = pair(x[i], x[i + stride])
                        if (base + i) >> phase & 1:
                            a, b = b, a
                        x[i], x[i + stride] = a, b
                stride //= 2
        for i in range(half):
            cs[base + i], ks[base + i] = x[i]
    merge_vregs(cs, ks, turned(vbits, vbits) ^ turned(vbits + 1, vbits))
    merge_phases(cs, ks, vbits + 1)


def merge_phases(cs, ks, begin):
    v = cs.shape[0]
    vbits = v.bit_length() - 1
    total = vbits + 10
    lane = lane_of()
    sub = sub_of()

    def sub_stage(j):
        step = 1 << j
        high = (sub & step) != 0

        def partner(x):
            up = pltpu.roll(x, step, 0)
            if step * 2 == SUBS:
                return up
            return jnp.where(high, up, pltpu.roll(x, SUBS - step, 0))

        for i in range(v):
            c, k = cs[i], ks[i]
            cs[i], ks[i] = exchange(c, k, partner(c), partner(k), high)

    def lane_stage(n, bits):
        step = jnp.int32(1) << (bits - 1 - n)
        high = (lane & step) != 0
        source = lane ^ step

        def partner(x):
            return jnp.take_along_axis(x, source, axis=1, mode="promise_in_bounds")

        for i in range(v):
            c, k = cs[i], ks[i]
            cs[i], ks[i] = exchange(c, k, partner(c), partner(k), high)
        return bits

    def phase_body(phase, carry):
        bits = jnp.maximum(phase - vbits - 3, 0)
        lax.fori_loop(0, bits, lane_stage, bits)
        for j in (2, 1, 0):
            if begin - vbits - 1 >= j:
                sub_stage(j)
            else:
                pl.when(phase - vbits - 1 >= j)(functools.partial(sub_stage, j))
        merge_vregs(cs, ks, turned(phase, vbits) ^ turned(phase + 1, vbits))
        return carry

    lax.fori_loop(begin, total + 1, phase_body, 0)


def earlier(x, q):
    y = pltpu.roll(x, q, 0)
    return jnp.where(sub_of() < q, pltpu.roll(y, 1, 1), y)


def later(x, q):
    y = pltpu.roll(x, SUBS - q, 0)
    return jnp.where(sub_of() >= SUBS - q, pltpu.roll(y, LANES - 1, 1), y)


def compress(limit, cs, ks, ds, cs2, ks2, ds2):
    v = cs.shape[0]
    vbits = v.bit_length() - 1
    lane = lane_of()
    sub = sub_of()
    start = (lane == 0) & (sub == 0)
    count = jnp.zeros((SUBS, LANES), jnp.int32)
    last = jnp.where(start, FAIL, earlier(cs[v - 1], 1))
    for i in range(v):
        c = cs[i]
        lost = (c == last) | (c < 0) | (c >= limit)
        ds[i] = jnp.where(lost, -1, count)
        count = count + lost.astype(jnp.int32)
        last = c
    scan = count
    for q in (1, 2, 4):
        scan = scan + jnp.where(sub >= q, pltpu.roll(scan, q, 0), 0)
    column = jnp.broadcast_to(scan[SUBS - 1 : SUBS, :], (SUBS, LANES))
    run = column
    for q in (1, 2, 4, 8, 16, 32, 64):
        run = run + jnp.where(lane >= q, pltpu.roll(run, q, 1), 0)
    offset = run - column + scan - count
    for i in range(v):
        d = ds[i]
        cs[i] = jnp.where(d < 0, NONE, cs[i])
        ds[i] = jnp.where(d < 0, 0, d + offset)

    def step(own, inc, bit):
        c, k, d = own
        pc, pk, pd = inc
        comes = (pd & bit) != 0
        goes = (d & bit) != 0
        return (
            jnp.where(comes, pc, jnp.where(goes, NONE, c)),
            jnp.where(comes, pk, k),
            jnp.where(comes, pd, jnp.where(goes, 0, d)),
        )

    now, then = (cs, ks, ds), (cs2, ks2, ds2)
    for b in range(vbits):
        for i in range(v):
            j = i + (1 << b)
            own = tuple(r[i] for r in now)
            inc = tuple(r[j] if j < v else later(r[j - v], 1) for r in now)
            for r, x in zip(then, step(own, inc, 1 << b)):
                r[i] = x
        now, then = then, now
    for b in range(3):
        for i in range(v):
            own = tuple(r[i] for r in now)
            inc = tuple(later(x, 1 << b) for x in own)
            for r, x in zip(now, step(own, inc, 1 << (b + vbits))):
                r[i] = x

    def lane_step(b, carry):
        shift = LANES - (jnp.int32(1) << b)
        for i in range(v):
            own = tuple(r[i] for r in now)
            inc = tuple(pltpu.roll(x, shift, 1) for x in own)
            for r, x in zip(now, step(own, inc, jnp.int32(1) << (b + vbits + 3))):
                r[i] = x
        return carry

    lax.fori_loop(0, 7, lane_step, 0)
    return now, then


def expand(ks, ds, ks2, ds2):
    v = ks.shape[0]
    vbits = v.bit_length() - 1

    def step(own, inc, bit):
        k, d = own
        pk, pd = inc
        comes = (pd & bit) != 0
        goes = (d & bit) != 0
        return (
            jnp.where(comes, pk, jnp.where(goes, EMPTY, k)),
            jnp.where(comes, pd, jnp.where(goes, 0, d)),
        )

    now, then = (ks, ds), (ks2, ds2)

    def lane_step(n, carry):
        b = 6 - n
        for i in range(v):
            own = tuple(r[i] for r in now)
            inc = tuple(pltpu.roll(x, jnp.int32(1) << b, 1) for x in own)
            for r, x in zip(now, step(own, inc, jnp.int32(1) << (b + vbits + 3))):
                r[i] = x
        return carry

    lax.fori_loop(0, 7, lane_step, 0)
    for b in (2, 1, 0):
        for i in range(v):
            own = tuple(r[i] for r in now)
            inc = tuple(earlier(x, 1 << b) for x in own)
            for r, x in zip(now, step(own, inc, 1 << (b + vbits))):
                r[i] = x
    for b in reversed(range(vbits)):
        for i in range(v):
            j = i - (1 << b)
            own = tuple(r[i] for r in now)
            inc = tuple(r[j] if j >= 0 else earlier(r[j + v], 1) for r in now)
            for r, x in zip(then, step(own, inc, 1 << b)):
                r[i] = x
        now, then = then, now
    return now[0]


def myself():
    return lax.axis_index("gx") * lax.axis_size("gy") + lax.axis_index("gy")


def flat(x, tall, out):
    v = x.shape[0]
    parts = v * SUBS // LANES
    for i in range(v):
        tall[pl.Slice(i, SUBS, v), :] = x[i]
    for h in range(parts):
        out[pl.Slice(h, LANES, parts), :] = jnp.transpose(tall[h * LANES : (h + 1) * LANES, :])


def send_kernel(n, cell_ref, vehicle_ref, speed_ref, out_ref, cs, ks, ds, cs2, ks2, ds2, tall, tc, tk):
    v = cs.shape[0]
    own = CELLS // n
    odd = myself() & 1
    for i in range(v):
        c = cell_ref[i]
        cs[i] = jnp.where(odd == 1, CELLS - 1 - c, c)
        ks[i] = encode(speed_ref[i], vehicle_ref[i])
    sort(cs, ks)
    (c, k, _), _ = compress(CELLS, cs, ks, ds, cs2, ks2, ds2)
    flat(c, tall, tc)
    flat(k, tall, tk)
    heads = LANES // v
    lead = [c[0][s : s + 1, :] for s in range(0, SUBS, heads)]
    tc[v * SUBS : (v + 1) * SUBS, :] = jnp.full((SUBS, LANES), NONE, jnp.int32)
    starts = []
    offs = []
    for q in range(n + 1):
        ahead = sum((x < q * own).astype(jnp.int32) for x in lead)
        starts.append(jnp.maximum(jnp.sum(ahead) - 1, 0))
    for q in range(n + 1):
        row = tc[pl.ds(starts[q], 1), :]
        offs.append(jnp.sum((row < q * own).astype(jnp.int32)))
    fails = jnp.int32(0)
    for q in range(n):
        size = (starts[q + 1] - starts[q]) * LANES + offs[q + 1] - offs[q]
        fails = fails | (size > ROWS * LANES).astype(jnp.int32)
    lane = lane_of()
    for q in range(n):
        o = jnp.where(odd == 1, n - 1 - q, q)
        tail = lane >= LANES - offs[q]

        def window(ref):
            x = pltpu.roll(ref[pl.ds(starts[q], SUBS), :], (LANES - offs[q]) & (LANES - 1), 1)
            return jnp.where(tail, pltpu.roll(x, SUBS - 1, 0), x)

        c = window(tc)
        k = jnp.where(c >= NONE, 0, window(tk))
        c = jnp.where(odd == 1, CELLS - 1 - c, c)
        c = jnp.where(fails > 0, FAIL, c)
        for at, w in enumerate(ORDER):
            out_ref[o, at : at + 1, :] = c[w : w + 1, :]
            out_ref[o, ROWS + at : ROWS + at + 1, :] = TOP - (k[w : w + 1, :] >> 10)
            out_ref[o, 2 * ROWS + at : 2 * ROWS + at + 1, :] = k[w : w + 1, :] & (UNIT - 1)
        out_ref[o, 3 * ROWS : 3 * ROWS + 1, :] = c[0:1, :]


def swap_kernel(n, sent, got, send_sem, recv_sem):
    me = myself()
    inner = lax.axis_size("gy")

    def spot(device):
        return (device // inner, device % inner)

    barrier = pltpu.get_barrier_semaphore()
    for k in range(1, n):
        pl.semaphore_signal(barrier, inc=1, device_id=spot(me ^ k), device_id_type=pl.DeviceIdType.MESH)
    mine = pltpu.make_async_copy(sent.at[me], got.at[me], send_sem.at[0])
    mine.start()
    pl.semaphore_wait(barrier, n - 1)
    copies = []
    for k in range(1, n):
        copy = pltpu.make_async_remote_copy(
            src_ref=sent.at[me ^ k],
            dst_ref=got.at[me],
            send_sem=send_sem.at[k],
            recv_sem=recv_sem.at[k],
            device_id=spot(me ^ k),
            device_id_type=pl.DeviceIdType.MESH,
        )
        copy.start()
        copies.append(copy)
    mine.wait()
    for copy in copies:
        copy.wait()


def owner_kernel(n, got_ref, speed_ref, vehicle_ref, fail_ref, cs, ks, ds, cs2, ks2, ds2, tall, uc, uk):
    v = cs.shape[0]
    vbits = v.bit_length() - 1
    own = CELLS // n
    base = myself() * own
    begin = vbits + 3 + WIDE.bit_length()
    flip = turned(begin, vbits)
    parts = v * SUBS // LANES
    least = jnp.zeros((1, LANES), jnp.int32)
    edge = lax.broadcasted_iota(jnp.int32, (v * WIDE, LANES), 0)
    pad = jnp.where((edge // WIDE) % 2 == 1, -NONE, NONE)
    for h in range(parts):
        uc[h] = pad
        uk[h] = jnp.zeros_like(pad)
    first = ROWS - ROWS // 2
    for o in range(n):
        c = got_ref[o, 0:ROWS, :]
        k = (TOP - got_ref[o, ROWS : 2 * ROWS, :]) * UNIT + got_ref[o, 2 * ROWS : 3 * ROWS, :]
        least = jnp.minimum(least, c[0:1, :])
        c = c - base
        uc[0, o * WIDE : o * WIDE + first, :] = c[0:first]
        uk[0, o * WIDE : o * WIDE + first, :] = k[0:first]
        uc[1, o * WIDE : o * WIDE + ROWS - first, :] = c[first:ROWS]
        uk[1, o * WIDE : o * WIDE + ROWS - first, :] = k[first:ROWS]
    for ref, out in ((uc, cs), (uk, ks)):
        for h in range(parts):
            tall[h * LANES : (h + 1) * LANES, :] = jnp.transpose(ref[h])
        for i in range(v):
            out[i] = tall[pl.Slice(i, SUBS, v), :] ^ flip
    fail_ref[0] = (jnp.min(least) == FAIL).astype(jnp.int32)
    merge_phases(cs, ks, begin)
    (c, k, d), (_, k2, d2) = compress(own, cs, ks, ds, cs2, ks2, ds2)
    place = (lane_of() * SUBS + sub_of()) * v
    for i in range(v):
        empty = c[i] >= NONE
        d[i] = jnp.where(empty, 0, c[i] - (place + i))
        k[i] = jnp.where(empty, EMPTY, k[i])
    done = expand(k, d, k2, d2)
    for i in range(v):
        tall[pl.Slice(i, SUBS, v), :] = done[i]
    columns = own // (v * SUBS)
    parts = v * SUBS // LANES
    wide = jnp.transpose(tall[...])
    for h in range(parts):
        speed, vehicle = finish(wide[0:columns, h * LANES : (h + 1) * LANES])
        speed_ref[pl.Slice(h, columns, parts), :] = speed
        vehicle_ref[pl.Slice(h, columns, parts), :] = vehicle


def sparse(cell, vehicle, speed, n):
    v = cell.shape[0] // (SUBS * LANES)
    own = CELLS // n
    shape = (v, SUBS, LANES)
    slots = [pltpu.VMEM(shape, jnp.int32)] * 6
    tall = pltpu.VMEM((v * SUBS, LANES), jnp.int32)
    rows = pltpu.VMEM(((v + 1) * SUBS, LANES), jnp.int32)
    runs = pltpu.VMEM((v * SUBS // LANES, v * WIDE, LANES), jnp.int32)
    sent = pl.pallas_call(
        functools.partial(send_kernel, n),
        out_shape=jax.ShapeDtypeStruct((n, 2 * SUBS, LANES), jnp.int32),
        scratch_shapes=slots + [tall, rows, rows],
    )(cell.reshape(shape), vehicle.reshape(shape), speed.reshape(shape))
    got = pl.pallas_call(
        functools.partial(swap_kernel, n),
        out_shape=jax.ShapeDtypeStruct(sent.shape, sent.dtype),
        in_specs=[pl.BlockSpec(memory_space=pltpu.VMEM)],
        out_specs=pl.BlockSpec(memory_space=pltpu.VMEM),
        scratch_shapes=[
            pltpu.SemaphoreType.DMA((n,)),
            pltpu.SemaphoreType.DMA((n,)),
        ],
        compiler_params=pltpu.CompilerParams(collective_id=0, has_side_effects=True),
    )(sent)
    best, ident, fail = pl.pallas_call(
        functools.partial(owner_kernel, n),
        out_shape=(
            jax.ShapeDtypeStruct((own // LANES, LANES), jnp.float32),
            jax.ShapeDtypeStruct((own // LANES, LANES), jnp.int32),
            jax.ShapeDtypeStruct((1,), jnp.int32),
        ),
        out_specs=(
            pl.BlockSpec(memory_space=pltpu.VMEM),
            pl.BlockSpec(memory_space=pltpu.VMEM),
            pl.BlockSpec(memory_space=pltpu.SMEM),
        ),
        scratch_shapes=slots + [tall, runs, runs],
    )(got)
    return best.reshape(own), ident.reshape(own), fail[0] > 0


def per_device(cell, vehicle, speed):
    n = lax.axis_size("gx") * lax.axis_size("gy")
    v = cell.shape[0] // (SUBS * LANES)
    if v != n or v * WIDE != LANES or cell.shape[0] % (SUBS * LANES) or CELLS % (n * v * SUBS):
        return dense(cell, vehicle, speed)
    best, ident, failed = sparse(cell, vehicle, speed, n)
    return lax.cond(
        failed,
        lambda: dense(cell, vehicle, speed),
        lambda: (best, ident),
    )


def solution(mesh):
    placed = (P(("gx", "gy")), P(("gx", "gy")), P(("gx", "gy")))
    return jax.shard_map(
        per_device,
        mesh=mesh,
        in_specs=placed,
        out_specs=(P(("gx", "gy")), P(("gx", "gy"))),
        check_vma=False,
    )
```

```python
import functools

import jax
import jax.numpy as jnp
from jax import lax
from jax.experimental import pallas as pl
from jax.experimental.pallas import tpu as pltpu
from jax.sharding import PartitionSpec as P

CELLS = 524288
TOP = 65536
UNIT = 1024
EMPTY = (TOP + UNIT) * UNIT
NONE = 1 << 30
FAIL = -2000000000
SUBS = 8
LANES = 128
GRANT = 16 << 20
WIDE = 4
ROWS = 5
ORDER = (0, 2, 4, 1, 3)


def swapped(block, axis, apart):
    count = lax.axis_size(axis)
    route = []
    for low in range(count):
        high = low | 1 << apart
        if high != low and high < count:
            route += [(low, high), (high, low)]
    return lax.ppermute(block, axis, route)


def encode(speed, vehicle):
    return (TOP - (speed * UNIT).astype(jnp.int32)) * UNIT + vehicle


def decode(code):
    level = TOP - (code >> 10)
    return level.astype(jnp.float32) * (1.0 / UNIT), code & (UNIT - 1)


def finish(code):
    speed, vehicle = decode(code)
    return speed, jnp.where(speed < 0, -1, vehicle)


def dense(cell, vehicle, speed):
    code = encode(speed, vehicle)
    buffer = jnp.full((CELLS,), EMPTY, jnp.int32).at[cell].min(code)
    outer = lax.axis_size("gx")
    inner = lax.axis_size("gy")
    nbits = (outer * inner).bit_length() - 1
    myself = lax.axis_index(("gx", "gy"))
    for level in reversed(range(nbits)):
        half = buffer.shape[0] // 2
        side = myself >> level & 1
        keep = lax.dynamic_slice_in_dim(buffer, side * half, half, 0)
        give = lax.dynamic_slice_in_dim(buffer, (1 - side) * half, half, 0)
        speed, vehicle = decode(give)
        partner = swapped(jnp.stack([speed, vehicle.astype(jnp.float32)]), ("gx", "gy"), level)
        buffer = jnp.minimum(keep, encode(partner[0], partner[1].astype(jnp.int32)))
    return finish(buffer)


def lane_of():
    return lax.broadcasted_iota(jnp.int32, (SUBS, LANES), 1)


def sub_of():
    return lax.broadcasted_iota(jnp.int32, (SUBS, LANES), 0)


def before(c, k, pc, pk):
    return (c < pc) | ((c == pc) & (k < pk))


def exchange(c, k, pc, pk, high):
    keep = jnp.logical_xor(before(c, k, pc, pk), high)
    return jnp.where(keep, c, pc), jnp.where(keep, k, pk)


def pair(x, y):
    swap = before(y[0], y[1], x[0], x[1])
    low = jnp.where(swap, y[0], x[0]), jnp.where(swap, y[1], x[1])
    high = jnp.where(swap, x[0], y[0]), jnp.where(swap, x[1], y[1])
    return low, high


def turned(bit, vbits):
    place = lane_of() * SUBS + sub_of()
    return -((place >> (bit - vbits)) & 1)


def merge_vregs(cs, ks, flip):
    v = cs.shape[0]
    half = v // 2
    for i in range(half):
        a, b = pair((cs[i], ks[i]), (cs[i + half], ks[i + half]))
        cs[i], ks[i] = a
        cs[i + half], ks[i + half] = b
    for base in (0, half):
        x = [(cs[base + i], ks[base + i]) for i in range(half)]
        stride = half // 2
        while stride:
            for i in range(half):
                if not i & stride:
                    x[i], x[i + stride] = pair(x[i], x[i + stride])
            stride //= 2
        for i in range(half):
            cs[base + i] = x[i][0] ^ flip
            ks[base + i] = x[i][1] ^ flip


def sort(cs, ks):
    v = cs.shape[0]
    half = v // 2
    vbits = v.bit_length() - 1
    total = vbits + 10
    flip = turned(vbits, vbits)
    for base in (0, half):
        x = [(cs[base + i] ^ flip, ks[base + i] ^ flip) for i in range(half)]
        for phase in range(1, vbits):
            stride = 1 << (phase - 1)
            while stride:
                for i in range(half):
                    if not i & stride:
                        a, b = pair(x[i], x[i + stride])
                        if (base + i) >> phase & 1:
                            a, b = b, a
                        x[i], x[i + stride] = a, b
                stride //= 2
        for i in range(half):
            cs[base + i], ks[base + i] = x[i]
    merge_vregs(cs, ks, turned(vbits, vbits) ^ turned(vbits + 1, vbits))
    merge_phases(cs, ks, vbits + 1)


def merge_phases(cs, ks, begin):
    v = cs.shape[0]
    vbits = v.bit_length() - 1
    total = vbits + 10
    lane = lane_of()
    sub = sub_of()

    def sub_stage(j):
        step = 1 << j
        high = (sub & step) != 0

        def partner(x):
            up = pltpu.roll(x, step, 0)
            if step * 2 == SUBS:
                return up
            return jnp.where(high, up, pltpu.roll(x, SUBS - step, 0))

        for i in range(v):
            c, k = cs[i], ks[i]
            cs[i], ks[i] = exchange(c, k, partner(c), partner(k), high)

    def lane_stage(bit):
        step = 1 << bit
        high = (lane & step) != 0
        source = lane ^ step

        def partner(x):
            return jnp.take_along_axis(x, source, axis=1, mode="promise_in_bounds")

        for i in range(v):
            c, k = cs[i], ks[i]
            cs[i], ks[i] = exchange(c, k, partner(c), partner(k), high)

    for phase in range(begin, total + 1):
        for bit in reversed(range(phase - vbits - 3)):
            lane_stage(bit)
        for j in (2, 1, 0):
            if phase - vbits - 1 >= j:
                sub_stage(j)
        merge_vregs(cs, ks, turned(phase, vbits) ^ turned(phase + 1, vbits))


def earlier(x, q):
    y = pltpu.roll(x, q, 0)
    return jnp.where(sub_of() < q, pltpu.roll(y, 1, 1), y)


def later(x, q):
    y = pltpu.roll(x, SUBS - q, 0)
    return jnp.where(sub_of() >= SUBS - q, pltpu.roll(y, LANES - 1, 1), y)


def compress(limit, cs, ks, ds, cs2, ks2, ds2):
    v = cs.shape[0]
    vbits = v.bit_length() - 1
    lane = lane_of()
    sub = sub_of()
    start = (lane == 0) & (sub == 0)
    count = jnp.zeros((SUBS, LANES), jnp.int32)
    last = jnp.where(start, FAIL, earlier(cs[v - 1], 1))
    for i in range(v):
        c = cs[i]
        lost = (c == last) | (c < 0) | (c >= limit)
        ds[i] = jnp.where(lost, -1, count)
        count = count + lost.astype(jnp.int32)
        last = c
    scan = count
    for q in (1, 2, 4):
        scan = scan + jnp.where(sub >= q, pltpu.roll(scan, q, 0), 0)
    column = jnp.broadcast_to(scan[SUBS - 1 : SUBS, :], (SUBS, LANES))
    run = column
    for q in (1, 2, 4, 8, 16, 32, 64):
        run = run + jnp.where(lane >= q, pltpu.roll(run, q, 1), 0)
    offset = run - column + scan - count
    for i in range(v):
        d = ds[i]
        cs[i] = jnp.where(d < 0, NONE, cs[i])
        ds[i] = jnp.where(d < 0, 0, d + offset)

    def step(own, inc, bit):
        c, k, d = own
        pc, pk, pd = inc
        comes = (pd & bit) != 0
        goes = (d & bit) != 0
        return (
            jnp.where(comes, pc, jnp.where(goes, NONE, c)),
            jnp.where(comes, pk, k),
            jnp.where(comes, pd, jnp.where(goes, 0, d)),
        )

    now, then = (cs, ks, ds), (cs2, ks2, ds2)
    for b in range(vbits):
        for i in range(v):
            j = i + (1 << b)
            own = tuple(r[i] for r in now)
            inc = tuple(r[j] if j < v else later(r[j - v], 1) for r in now)
            for r, x in zip(then, step(own, inc, 1 << b)):
                r[i] = x
        now, then = then, now
    for b in range(3):
        for i in range(v):
            own = tuple(r[i] for r in now)
            inc = tuple(later(x, 1 << b) for x in own)
            for r, x in zip(now, step(own, inc, 1 << (b + vbits))):
                r[i] = x

    for b in range(7):
        shift = LANES - (1 << b)
        for i in range(v):
            own = tuple(r[i] for r in now)
            inc = tuple(pltpu.roll(x, shift, 1) for x in own)
            for r, x in zip(now, step(own, inc, 1 << (b + vbits + 3))):
                r[i] = x
    return now, then


def expand(ks, ds, ks2, ds2):
    v = ks.shape[0]
    vbits = v.bit_length() - 1

    def step(own, inc, bit):
        k, d = own
        pk, pd = inc
        comes = (pd & bit) != 0
        goes = (d & bit) != 0
        return (
            jnp.where(comes, pk, jnp.where(goes, EMPTY, k)),
            jnp.where(comes, pd, jnp.where(goes, 0, d)),
        )

    now, then = (ks, ds), (ks2, ds2)

    for b in reversed(range(7)):
        for i in range(v):
            own = tuple(r[i] for r in now)
            inc = tuple(pltpu.roll(x, 1 << b, 1) for x in own)
            for r, x in zip(now, step(own, inc, 1 << (b + vbits + 3))):
                r[i] = x
    for b in (2, 1, 0):
        for i in range(v):
            own = tuple(r[i] for r in now)
            inc = tuple(earlier(x, 1 << b) for x in own)
            for r, x in zip(now, step(own, inc, 1 << (b + vbits))):
                r[i] = x
    for b in reversed(range(vbits)):
        for i in range(v):
            j = i - (1 << b)
            own = tuple(r[i] for r in now)
            inc = tuple(r[j] if j >= 0 else earlier(r[j + v], 1) for r in now)
            for r, x in zip(then, step(own, inc, 1 << b)):
                r[i] = x
        now, then = then, now
    return now[0]


def myself():
    return lax.axis_index("gx") * lax.axis_size("gy") + lax.axis_index("gy")


def flat(x, tall, out):
    v = x.shape[0]
    parts = v * SUBS // LANES
    for i in range(v):
        tall[pl.Slice(i, SUBS, v), :] = x[i]
    for h in range(parts):
        out[pl.Slice(h, LANES, parts), :] = jnp.transpose(tall[h * LANES : (h + 1) * LANES, :])


def send_kernel(n, cell_ref, vehicle_ref, speed_ref, out_ref, cs, ks, ds, cs2, ks2, ds2, tall, tc, tk):
    v = cs.shape[0]
    own = CELLS // n
    odd = myself() & 1
    for i in range(v):
        c = cell_ref[i]
        cs[i] = jnp.where(odd == 1, CELLS - 1 - c, c)
        ks[i] = encode(speed_ref[i], vehicle_ref[i])
    sort(cs, ks)
    (c, k, _), _ = compress(CELLS, cs, ks, ds, cs2, ks2, ds2)
    flat(c, tall, tc)
    flat(k, tall, tk)
    heads = LANES // v
    lead = [c[0][s : s + 1, :] for s in range(0, SUBS, heads)]
    tc[v * SUBS : (v + 1) * SUBS, :] = jnp.full((SUBS, LANES), NONE, jnp.int32)
    starts = []
    offs = []
    for q in range(n + 1):
        ahead = sum((x < q * own).astype(jnp.int32) for x in lead)
        starts.append(jnp.maximum(jnp.sum(ahead) - 1, 0))
    for q in range(n + 1):
        row = tc[pl.ds(starts[q], 1), :]
        offs.append(jnp.sum((row < q * own).astype(jnp.int32)))
    fails = jnp.int32(0)
    for q in range(n):
        size = (starts[q + 1] - starts[q]) * LANES + offs[q + 1] - offs[q]
        fails = fails | (size > ROWS * LANES).astype(jnp.int32)
    lane = lane_of()
    for q in range(n):
        o = jnp.where(odd == 1, n - 1 - q, q)
        tail = lane >= LANES - offs[q]

        def window(ref):
            x = pltpu.roll(ref[pl.ds(starts[q], SUBS), :], (LANES - offs[q]) & (LANES - 1), 1)
            return jnp.where(tail, pltpu.roll(x, SUBS - 1, 0), x)

        c = window(tc)
        k = jnp.where(c >= NONE, 0, window(tk))
        c = jnp.where(odd == 1, CELLS - 1 - c, c)
        c = jnp.where(fails > 0, FAIL, c)
        for at, w in enumerate(ORDER):
            out_ref[o, at : at + 1, :] = c[w : w + 1, :]
            out_ref[o, ROWS + at : ROWS + at + 1, :] = TOP - (k[w : w + 1, :] >> 10)
            out_ref[o, 2 * ROWS + at : 2 * ROWS + at + 1, :] = k[w : w + 1, :] & (UNIT - 1)
        out_ref[o, 3 * ROWS : 3 * ROWS + 1, :] = c[0:1, :]


def swap_kernel(n, sent, got, send_sem, recv_sem):
    me = myself()
    inner = lax.axis_size("gy")

    def spot(device):
        return (device // inner, device % inner)

    barrier = pltpu.get_barrier_semaphore()
    for k in range(1, n):
        pl.semaphore_signal(barrier, inc=1, device_id=spot(me ^ k), device_id_type=pl.DeviceIdType.MESH)
    mine = pltpu.make_async_copy(sent.at[me], got.at[me], send_sem.at[0])
    mine.start()
    pl.semaphore_wait(barrier, n - 1)
    copies = []
    for k in sorted(range(1, n), key=lambda k: -(k % inner)):
        copy = pltpu.make_async_remote_copy(
            src_ref=sent.at[me ^ k],
            dst_ref=got.at[me],
            send_sem=send_sem.at[k],
            recv_sem=recv_sem.at[k],
            device_id=spot(me ^ k),
            device_id_type=pl.DeviceIdType.MESH,
        )
        copy.start()
        copies.append(copy)
    mine.wait()
    for copy in copies:
        copy.wait()


def owner_kernel(n, got_ref, speed_ref, vehicle_ref, fail_ref, cs, ks, ds, cs2, ks2, ds2, tall, uc, uk):
    v = cs.shape[0]
    vbits = v.bit_length() - 1
    own = CELLS // n
    base = myself() * own
    begin = vbits + 3 + WIDE.bit_length()
    flip = turned(begin, vbits)
    parts = v * SUBS // LANES
    least = jnp.zeros((1, LANES), jnp.int32)
    edge = lax.broadcasted_iota(jnp.int32, (v * WIDE, LANES), 0)
    pad = jnp.where((edge // WIDE) % 2 == 1, -NONE, NONE)
    for h in range(parts):
        uc[h] = pad
        uk[h] = jnp.zeros_like(pad)
    first = ROWS - ROWS // 2
    for o in range(n):
        c = got_ref[o, 0:ROWS, :]
        k = (TOP - got_ref[o, ROWS : 2 * ROWS, :]) * UNIT + got_ref[o, 2 * ROWS : 3 * ROWS, :]
        least = jnp.minimum(least, c[0:1, :])
        c = c - base
        uc[0, o * WIDE : o * WIDE + first, :] = c[0:first]
        uk[0, o * WIDE : o * WIDE + first, :] = k[0:first]
        uc[1, o * WIDE : o * WIDE + ROWS - first, :] = c[first:ROWS]
        uk[1, o * WIDE : o * WIDE + ROWS - first, :] = k[first:ROWS]
    for ref, out in ((uc, cs), (uk, ks)):
        for h in range(parts):
            tall[h * LANES : (h + 1) * LANES, :] = jnp.transpose(ref[h])
        for i in range(v):
            out[i] = tall[pl.Slice(i, SUBS, v), :] ^ flip
    fail_ref[0] = (jnp.min(least) == FAIL).astype(jnp.int32)
    merge_phases(cs, ks, begin)
    (c, k, d), (_, k2, d2) = compress(own, cs, ks, ds, cs2, ks2, ds2)
    place = (lane_of() * SUBS + sub_of()) * v
    for i in range(v):
        empty = c[i] >= NONE
        d[i] = jnp.where(empty, 0, c[i] - (place + i))
        k[i] = jnp.where(empty, EMPTY, k[i])
    done = expand(k, d, k2, d2)
    for i in range(v):
        tall[pl.Slice(i, SUBS, v), :] = done[i]
    columns = own // (v * SUBS)
    parts = v * SUBS // LANES
    wide = jnp.transpose(tall[...])
    for h in range(parts):
        speed, vehicle = finish(wide[0:columns, h * LANES : (h + 1) * LANES])
        speed_ref[pl.Slice(h, columns, parts), :] = speed
        vehicle_ref[pl.Slice(h, columns, parts), :] = vehicle


def sparse(cell, vehicle, speed, n):
    v = cell.shape[0] // (SUBS * LANES)
    own = CELLS // n
    shape = (v, SUBS, LANES)
    slots = [pltpu.VMEM(shape, jnp.int32)] * 6
    tall = pltpu.VMEM((v * SUBS, LANES), jnp.int32)
    rows = pltpu.VMEM(((v + 1) * SUBS, LANES), jnp.int32)
    runs = pltpu.VMEM((v * SUBS // LANES, v * WIDE, LANES), jnp.int32)
    sent = pl.pallas_call(
        functools.partial(send_kernel, n),
        out_shape=jax.ShapeDtypeStruct((n, 2 * SUBS, LANES), jnp.int32),
        compiler_params=pltpu.CompilerParams(vmem_limit_bytes=GRANT),
        scratch_shapes=slots + [tall, rows, rows],
    )(cell.reshape(shape), vehicle.reshape(shape), speed.reshape(shape))
    got = pl.pallas_call(
        functools.partial(swap_kernel, n),
        out_shape=jax.ShapeDtypeStruct(sent.shape, sent.dtype),
        in_specs=[pl.BlockSpec(memory_space=pltpu.VMEM)],
        out_specs=pl.BlockSpec(memory_space=pltpu.VMEM),
        scratch_shapes=[
            pltpu.SemaphoreType.DMA((n,)),
            pltpu.SemaphoreType.DMA((n,)),
        ],
        compiler_params=pltpu.CompilerParams(collective_id=0, has_side_effects=True, vmem_limit_bytes=GRANT),
    )(sent)
    best, ident, fail = pl.pallas_call(
        functools.partial(owner_kernel, n),
        out_shape=(
            jax.ShapeDtypeStruct((own // LANES, LANES), jnp.float32),
            jax.ShapeDtypeStruct((own // LANES, LANES), jnp.int32),
            jax.ShapeDtypeStruct((1,), jnp.int32),
        ),
        out_specs=(
            pl.BlockSpec(memory_space=pltpu.VMEM),
            pl.BlockSpec(memory_space=pltpu.VMEM),
            pl.BlockSpec(memory_space=pltpu.SMEM),
        ),
        compiler_params=pltpu.CompilerParams(vmem_limit_bytes=GRANT),
        scratch_shapes=slots + [tall, runs, runs],
    )(got)
    return best.reshape(own), ident.reshape(own), fail[0] > 0


def per_device(cell, vehicle, speed):
    n = lax.axis_size("gx") * lax.axis_size("gy")
    v = cell.shape[0] // (SUBS * LANES)
    if v != n or v * WIDE != LANES or cell.shape[0] % (SUBS * LANES) or CELLS % (n * v * SUBS):
        return dense(cell, vehicle, speed)
    best, ident, failed = sparse(cell, vehicle, speed, n)
    return lax.cond(
        failed,
        lambda: dense(cell, vehicle, speed),
        lambda: (best, ident),
    )


def solution(mesh):
    placed = (P(("gx", "gy")), P(("gx", "gy")), P(("gx", "gy")))
    return jax.shard_map(
        per_device,
        mesh=mesh,
        in_specs=placed,
        out_specs=(P(("gx", "gy")), P(("gx", "gy"))),
        check_vma=False,
    )
```

```python
import functools

import jax
import jax.numpy as jnp
from jax import lax
from jax.experimental import pallas as pl
from jax.experimental.pallas import tpu as pltpu
from jax.sharding import PartitionSpec as P

CELLS = 524288
TOP = 65536
UNIT = 1024
EMPTY = (TOP + UNIT) * UNIT
NONE = 1 << 30
FAIL = -2000000000
GAP = 1 << 19
SUBS = 8
LANES = 128
GRANT = 16 << 20
WIDE = 4
ROWS = 5
ORDER = (0, 2, 4, 1, 3)


def swapped(block, axis, apart):
    count = lax.axis_size(axis)
    route = []
    for low in range(count):
        high = low | 1 << apart
        if high != low and high < count:
            route += [(low, high), (high, low)]
    return lax.ppermute(block, axis, route)


def encode(speed, vehicle):
    return (TOP - (speed * UNIT).astype(jnp.int32)) * UNIT + vehicle


def decode(code):
    level = TOP - (code >> 10)
    return level.astype(jnp.float32) * (1.0 / UNIT), code & (UNIT - 1)


def finish(code):
    speed, vehicle = decode(code)
    return speed, jnp.where(speed < 0, -1, vehicle)


def dense(cell, vehicle, speed):
    code = encode(speed, vehicle)
    buffer = jnp.full((CELLS,), EMPTY, jnp.int32).at[cell].min(code)
    outer = lax.axis_size("gx")
    inner = lax.axis_size("gy")
    nbits = (outer * inner).bit_length() - 1
    myself = lax.axis_index(("gx", "gy"))
    for level in reversed(range(nbits)):
        half = buffer.shape[0] // 2
        side = myself >> level & 1
        keep = lax.dynamic_slice_in_dim(buffer, side * half, half, 0)
        give = lax.dynamic_slice_in_dim(buffer, (1 - side) * half, half, 0)
        speed, vehicle = decode(give)
        partner = swapped(jnp.stack([speed, vehicle.astype(jnp.float32)]), ("gx", "gy"), level)
        buffer = jnp.minimum(keep, encode(partner[0], partner[1].astype(jnp.int32)))
    return finish(buffer)


def lane_of():
    return lax.broadcasted_iota(jnp.int32, (SUBS, LANES), 1)


def sub_of():
    return lax.broadcasted_iota(jnp.int32, (SUBS, LANES), 0)


def before(c, k, pc, pk):
    return (c < pc) | ((c == pc) & (k < pk))


def exchange(c, k, pc, pk, high):
    keep = jnp.logical_xor(before(c, k, pc, pk), high)
    return jnp.where(keep, c, pc), jnp.where(keep, k, pk)


def pair(x, y):
    swap = before(y[0], y[1], x[0], x[1])
    low = jnp.where(swap, y[0], x[0]), jnp.where(swap, y[1], x[1])
    high = jnp.where(swap, x[0], y[0]), jnp.where(swap, x[1], y[1])
    return low, high


def turned(bit, vbits):
    place = lane_of() * SUBS + sub_of()
    return -((place >> (bit - vbits)) & 1)


def merge_vregs(cs, ks, flip):
    v = cs.shape[0]
    half = v // 2
    for i in range(half):
        a, b = pair((cs[i], ks[i]), (cs[i + half], ks[i + half]))
        cs[i], ks[i] = a
        cs[i + half], ks[i + half] = b
    for base in (0, half):
        x = [(cs[base + i], ks[base + i]) for i in range(half)]
        stride = half // 2
        while stride:
            for i in range(half):
                if not i & stride:
                    x[i], x[i + stride] = pair(x[i], x[i + stride])
            stride //= 2
        for i in range(half):
            cs[base + i] = x[i][0] ^ flip
            ks[base + i] = x[i][1] ^ flip


def sort(cs, ks):
    v = cs.shape[0]
    half = v // 2
    vbits = v.bit_length() - 1
    total = vbits + 10
    flip = turned(vbits, vbits)
    for base in (0, half):
        x = [(cs[base + i] ^ flip, ks[base + i] ^ flip) for i in range(half)]
        for phase in range(1, vbits):
            stride = 1 << (phase - 1)
            while stride:
                for i in range(half):
                    if not i & stride:
                        a, b = pair(x[i], x[i + stride])
                        if (base + i) >> phase & 1:
                            a, b = b, a
                        x[i], x[i + stride] = a, b
                stride //= 2
        for i in range(half):
            cs[base + i], ks[base + i] = x[i]
    merge_vregs(cs, ks, turned(vbits, vbits) ^ turned(vbits + 1, vbits))
    merge_phases(cs, ks, vbits + 1)


def merge_phases(cs, ks, begin):
    v = cs.shape[0]
    vbits = v.bit_length() - 1
    total = vbits + 10
    lane = lane_of()
    sub = sub_of()

    def sub_stage(j):
        step = 1 << j
        high = (sub & step) != 0

        def partner(x):
            up = pltpu.roll(x, step, 0)
            if step * 2 == SUBS:
                return up
            return jnp.where(high, up, pltpu.roll(x, SUBS - step, 0))

        for i in range(v):
            c, k = cs[i], ks[i]
            cs[i], ks[i] = exchange(c, k, partner(c), partner(k), high)

    def lane_stage(bit):
        step = 1 << bit
        high = (lane & step) != 0
        source = lane ^ step

        def partner(x):
            return jnp.take_along_axis(x, source, axis=1, mode="promise_in_bounds")

        for i in range(v):
            c, k = cs[i], ks[i]
            cs[i], ks[i] = exchange(c, k, partner(c), partner(k), high)

    for phase in range(begin, total + 1):
        for bit in reversed(range(phase - vbits - 3)):
            lane_stage(bit)
        for j in (2, 1, 0):
            if phase - vbits - 1 >= j:
                sub_stage(j)
        merge_vregs(cs, ks, turned(phase, vbits) ^ turned(phase + 1, vbits))


def earlier(x, q):
    y = pltpu.roll(x, q, 0)
    return jnp.where(sub_of() < q, pltpu.roll(y, 1, 1), y)


def later(x, q):
    y = pltpu.roll(x, SUBS - q, 0)
    return jnp.where(sub_of() >= SUBS - q, pltpu.roll(y, LANES - 1, 1), y)


def compress(limit, cs, ks, ds, cs2, ks2, ds2):
    v = cs.shape[0]
    vbits = v.bit_length() - 1
    lane = lane_of()
    sub = sub_of()
    start = (lane == 0) & (sub == 0)
    count = jnp.zeros((SUBS, LANES), jnp.int32)
    last = jnp.where(start, FAIL, earlier(cs[v - 1], 1))
    for i in range(v):
        c = cs[i]
        lost = (c == last) | (c < 0) | (c >= limit)
        ds[i] = jnp.where(lost, -1, count)
        count = count + lost.astype(jnp.int32)
        last = c
    scan = count
    for q in (1, 2, 4):
        scan = scan + jnp.where(sub >= q, pltpu.roll(scan, q, 0), 0)
    column = jnp.broadcast_to(scan[SUBS - 1 : SUBS, :], (SUBS, LANES))
    run = column
    for q in (1, 2, 4, 8, 16, 32, 64):
        run = run + jnp.where(lane >= q, pltpu.roll(run, q, 1), 0)
    offset = run - column + scan - count
    for i in range(v):
        d = ds[i]
        lost = d < 0
        d = d + offset
        cs[i] = jnp.where(lost, GAP, (d >> 4 << 20) | cs[i])
        ks[i] = jnp.where(lost, 0, ((d & 15) << 27) | ks[i])

    def step(own, inc, b):
        c, k = own
        pc, pk = inc
        word, bit = (1, 1 << (27 + b)) if b < 4 else (0, 1 << (16 + b))
        comes = (inc[word] & bit) != 0
        goes = (own[word] & bit) != 0
        return (
            jnp.where(comes, pc, jnp.where(goes, GAP, c)),
            jnp.where(comes, pk, jnp.where(goes, 0, k)),
        )

    now, then = (cs, ks), (cs2, ks2)
    for b in range(vbits):
        for i in range(v):
            j = i + (1 << b)
            own = tuple(r[i] for r in now)
            inc = tuple(r[j] if j < v else later(r[j - v], 1) for r in now)
            for r, x in zip(then, step(own, inc, b)):
                r[i] = x
        now, then = then, now
    for b in range(10):
        for i in range(v):
            own = tuple(r[i] for r in now)
            if b < 3:
                inc = tuple(later(x, 1 << b) for x in own)
            else:
                inc = tuple(pltpu.roll(x, LANES - (1 << (b - 3)), 1) for x in own)
            c, k = step(own, inc, b + vbits)
            if b == 9:
                c = c & (2 * GAP - 1)
                c = jnp.where(c == GAP, NONE, c)
                k = k & ((1 << 27) - 1)
            now[0][i] = c
            now[1][i] = k
    return now + (ds,), then + (ds2,)


def expand(ks, ds, ks2, ds2):
    v = ks.shape[0]
    vbits = v.bit_length() - 1

    def step(own, inc, bit):
        k, d = own
        pk, pd = inc
        comes = (pd & bit) != 0
        goes = (d & bit) != 0
        return (
            jnp.where(comes, pk, jnp.where(goes, EMPTY, k)),
            jnp.where(comes, pd, jnp.where(goes, 0, d)),
        )

    now, then = (ks, ds), (ks2, ds2)

    for b in reversed(range(7)):
        for i in range(v):
            own = tuple(r[i] for r in now)
            inc = tuple(pltpu.roll(x, 1 << b, 1) for x in own)
            for r, x in zip(now, step(own, inc, 1 << (b + vbits + 3))):
                r[i] = x
    for b in (2, 1, 0):
        for i in range(v):
            own = tuple(r[i] for r in now)
            inc = tuple(earlier(x, 1 << b) for x in own)
            for r, x in zip(now, step(own, inc, 1 << (b + vbits))):
                r[i] = x
    for b in reversed(range(vbits)):
        for i in range(v):
            j = i - (1 << b)
            own = tuple(r[i] for r in now)
            inc = tuple(r[j] if j >= 0 else earlier(r[j + v], 1) for r in now)
            for r, x in zip(then, step(own, inc, 1 << b)):
                r[i] = x
        now, then = then, now
    return now[0]


def myself():
    return lax.axis_index("gx") * lax.axis_size("gy") + lax.axis_index("gy")


def flat(x, tall, out):
    v = x.shape[0]
    parts = v * SUBS // LANES
    for i in range(v):
        tall[pl.Slice(i, SUBS, v), :] = x[i]
    for h in range(parts):
        out[pl.Slice(h, LANES, parts), :] = jnp.transpose(tall[h * LANES : (h + 1) * LANES, :])


def send_kernel(n, cell_ref, vehicle_ref, speed_ref, out_ref, cs, ks, ds, cs2, ks2, ds2, tall, tc, tk):
    v = cs.shape[0]
    own = CELLS // n
    odd = myself() & 1
    for i in range(v):
        c = cell_ref[i]
        cs[i] = jnp.where(odd == 1, CELLS - 1 - c, c)
        ks[i] = encode(speed_ref[i], vehicle_ref[i])
    sort(cs, ks)
    (c, k, _), _ = compress(CELLS, cs, ks, ds, cs2, ks2, ds2)
    flat(c, tall, tc)
    flat(k, tall, tk)
    heads = LANES // v
    lead = [c[0][s : s + 1, :] for s in range(0, SUBS, heads)]
    tc[v * SUBS : (v + 1) * SUBS, :] = jnp.full((SUBS, LANES), NONE, jnp.int32)
    starts = []
    offs = []
    for q in range(n + 1):
        ahead = sum((x < q * own).astype(jnp.int32) for x in lead)
        starts.append(jnp.maximum(jnp.sum(ahead) - 1, 0))
    for q in range(n + 1):
        row = tc[pl.ds(starts[q], 1), :]
        offs.append(jnp.sum((row < q * own).astype(jnp.int32)))
    fails = jnp.int32(0)
    for q in range(n):
        size = (starts[q + 1] - starts[q]) * LANES + offs[q + 1] - offs[q]
        fails = fails | (size > ROWS * LANES).astype(jnp.int32)
    lane = lane_of()
    for q in range(n):
        o = jnp.where(odd == 1, n - 1 - q, q)
        tail = lane >= LANES - offs[q]

        def window(ref):
            x = pltpu.roll(ref[pl.ds(starts[q], SUBS), :], (LANES - offs[q]) & (LANES - 1), 1)
            return jnp.where(tail, pltpu.roll(x, SUBS - 1, 0), x)

        c = window(tc)
        k = jnp.where(c >= NONE, 0, window(tk))
        c = jnp.where(odd == 1, CELLS - 1 - c, c)
        c = jnp.where(fails > 0, FAIL, c)
        for at, w in enumerate(ORDER):
            out_ref[o, at : at + 1, :] = c[w : w + 1, :]
            out_ref[o, ROWS + at : ROWS + at + 1, :] = TOP - (k[w : w + 1, :] >> 10)
            out_ref[o, 2 * ROWS + at : 2 * ROWS + at + 1, :] = k[w : w + 1, :] & (UNIT - 1)
        out_ref[o, 3 * ROWS : 3 * ROWS + 1, :] = c[0:1, :]


def swap_kernel(n, sent, got, send_sem, recv_sem):
    me = myself()
    inner = lax.axis_size("gy")

    def spot(device):
        return (device // inner, device % inner)

    barrier = pltpu.get_barrier_semaphore()
    for k in range(1, n):
        pl.semaphore_signal(barrier, inc=1, device_id=spot(me ^ k), device_id_type=pl.DeviceIdType.MESH)
    mine = pltpu.make_async_copy(sent.at[me], got.at[me], send_sem.at[0])
    mine.start()
    pl.semaphore_wait(barrier, n - 1)
    copies = []
    for k in sorted(range(1, n), key=lambda k: -(k % inner)):
        copy = pltpu.make_async_remote_copy(
            src_ref=sent.at[me ^ k, 0 : 3 * ROWS],
            dst_ref=got.at[me, 0 : 3 * ROWS],
            send_sem=send_sem.at[k],
            recv_sem=recv_sem.at[k],
            device_id=spot(me ^ k),
            device_id_type=pl.DeviceIdType.MESH,
        )
        copy.start()
        copies.append(copy)
    mine.wait()
    for copy in copies:
        copy.wait()


def owner_kernel(n, got_ref, speed_ref, vehicle_ref, fail_ref, cs, ks, ds, cs2, ks2, ds2, tall, uc, uk):
    v = cs.shape[0]
    vbits = v.bit_length() - 1
    own = CELLS // n
    base = myself() * own
    begin = vbits + 3 + WIDE.bit_length()
    flip = turned(begin, vbits)
    parts = v * SUBS // LANES
    least = jnp.zeros((1, LANES), jnp.int32)
    edge = lax.broadcasted_iota(jnp.int32, (v * WIDE, LANES), 0)
    pad = jnp.where((edge // WIDE) % 2 == 1, -NONE, NONE)
    for h in range(parts):
        uc[h] = pad
        uk[h] = jnp.zeros_like(pad)
    first = ROWS - ROWS // 2
    for o in range(n):
        c = got_ref[o, 0:ROWS, :]
        k = (TOP - got_ref[o, ROWS : 2 * ROWS, :]) * UNIT + got_ref[o, 2 * ROWS : 3 * ROWS, :]
        least = jnp.minimum(least, c[0:1, :])
        c = c - base
        uc[0, o * WIDE : o * WIDE + first, :] = c[0:first]
        uk[0, o * WIDE : o * WIDE + first, :] = k[0:first]
        uc[1, o * WIDE : o * WIDE + ROWS - first, :] = c[first:ROWS]
        uk[1, o * WIDE : o * WIDE + ROWS - first, :] = k[first:ROWS]
    for ref, out in ((uc, cs), (uk, ks)):
        for h in range(parts):
            tall[h * LANES : (h + 1) * LANES, :] = jnp.transpose(ref[h])
        for i in range(v):
            out[i] = tall[pl.Slice(i, SUBS, v), :] ^ flip
    fail_ref[0] = (jnp.min(least) == FAIL).astype(jnp.int32)
    merge_phases(cs, ks, begin)
    (c, k, d), (_, k2, d2) = compress(own, cs, ks, ds, cs2, ks2, ds2)
    place = (lane_of() * SUBS + sub_of()) * v
    for i in range(v):
        empty = c[i] >= NONE
        d[i] = jnp.where(empty, 0, c[i] - (place + i))
        k[i] = jnp.where(empty, EMPTY, k[i])
    done = expand(k, d, k2, d2)
    for i in range(v):
        tall[pl.Slice(i, SUBS, v), :] = done[i]
    columns = own // (v * SUBS)
    parts = v * SUBS // LANES
    wide = jnp.transpose(tall[...])
    for h in range(parts):
        speed, vehicle = finish(wide[0:columns, h * LANES : (h + 1) * LANES])
        speed_ref[pl.Slice(h, columns, parts), :] = speed
        vehicle_ref[pl.Slice(h, columns, parts), :] = vehicle


def sparse(cell, vehicle, speed, n):
    v = cell.shape[0] // (SUBS * LANES)
    own = CELLS // n
    shape = (v, SUBS, LANES)
    slots = [pltpu.VMEM(shape, jnp.int32)] * 6
    tall = pltpu.VMEM((v * SUBS, LANES), jnp.int32)
    rows = pltpu.VMEM(((v + 1) * SUBS, LANES), jnp.int32)
    runs = pltpu.VMEM((v * SUBS // LANES, v * WIDE, LANES), jnp.int32)
    sent = pl.pallas_call(
        functools.partial(send_kernel, n),
        out_shape=jax.ShapeDtypeStruct((n, 2 * SUBS, LANES), jnp.int32),
        compiler_params=pltpu.CompilerParams(vmem_limit_bytes=GRANT),
        scratch_shapes=slots + [tall, rows, rows],
    )(cell.reshape(shape), vehicle.reshape(shape), speed.reshape(shape))
    got = pl.pallas_call(
        functools.partial(swap_kernel, n),
        out_shape=jax.ShapeDtypeStruct(sent.shape, sent.dtype),
        in_specs=[pl.BlockSpec(memory_space=pltpu.VMEM)],
        out_specs=pl.BlockSpec(memory_space=pltpu.VMEM),
        scratch_shapes=[
            pltpu.SemaphoreType.DMA((n,)),
            pltpu.SemaphoreType.DMA((n,)),
        ],
        compiler_params=pltpu.CompilerParams(collective_id=0, has_side_effects=True, vmem_limit_bytes=GRANT),
    )(sent)
    best, ident, fail = pl.pallas_call(
        functools.partial(owner_kernel, n),
        out_shape=(
            jax.ShapeDtypeStruct((own // LANES, LANES), jnp.float32),
            jax.ShapeDtypeStruct((own // LANES, LANES), jnp.int32),
            jax.ShapeDtypeStruct((1,), jnp.int32),
        ),
        out_specs=(
            pl.BlockSpec(memory_space=pltpu.VMEM),
            pl.BlockSpec(memory_space=pltpu.VMEM),
            pl.BlockSpec(memory_space=pltpu.SMEM),
        ),
        compiler_params=pltpu.CompilerParams(vmem_limit_bytes=GRANT),
        scratch_shapes=slots + [tall, runs, runs],
    )(got)
    return best.reshape(own), ident.reshape(own), fail[0] > 0


def per_device(cell, vehicle, speed):
    n = lax.axis_size("gx") * lax.axis_size("gy")
    v = cell.shape[0] // (SUBS * LANES)
    if v != n or v * WIDE != LANES or cell.shape[0] % (SUBS * LANES) or CELLS % (n * v * SUBS):
        return dense(cell, vehicle, speed)
    best, ident, failed = sparse(cell, vehicle, speed, n)
    return lax.cond(
        failed,
        lambda: dense(cell, vehicle, speed),
        lambda: (best, ident),
    )


def solution(mesh):
    placed = (P(("gx", "gy")), P(("gx", "gy")), P(("gx", "gy")))
    return jax.shard_map(
        per_device,
        mesh=mesh,
        in_specs=placed,
        out_specs=(P(("gx", "gy")), P(("gx", "gy"))),
        check_vma=False,
    )
```
